32 devices in a mesh: kx: 8 (over y, x, core), ky: 4 (over z).
Axes of the slice: x: 2, y: 2, z: 4, core: 2. Of those that a mesh axis runs over, the one named last changes fastest.
Arguments:
- coeffs: bfloat16 [8, 4, 2, 36, 128, 256], P('kx', 'ky'), may hold values from -1 to 1, as said below
- bands: int32 [32], replicated, may hold values from 0 to 35, as said below
- umklapp: int32 [2, 2], replicated, may hold values from -3 to 3
Outputs:
- flux: float32 [8, 4, 2], P('kx', 'ky')
- links: float32 [8, 4, 3, 2], P('kx', 'ky')
The draws below stay inside these ranges and needn't reach their ends.
Inputs may be any that keep to these rules, and one draw needn't show every extreme that they name: 32 different indices of stored bands. `coeffs`: coefficients of order 1 / sqrt(32768); link matrices between neighbouring k-points stay close enough to unitary that elimination without row exchanges has pivots of magnitude near one.
All inputs are finite; a program needn't handle non-finite values.
Results may differ from the reference program's by a relative error of at most 0.0003.
Values may be sent and summed in bfloat16 or wider, within the bound.
A program may use at most 128 MiB of HBM per device.

```python
import math
import jax
import jax.numpy as jnp
from jax import lax

GX = 128
GY = 256
NBAND = 32
NSTORE = 36
NKX = 8
NKY = 4


def draw_coeffs(key, part):
    gsize = GX * GY
    key_modes, key_mix, key_noise = jax.random.split(jax.random.fold_in(key, 11), 3)
    modes = jax.random.permutation(key_modes, gsize)[:NSTORE]
    freq_x = (modes // GY).astype(jnp.float32)
    freq_y = (modes % GY).astype(jnp.float32)
    grid_x = jnp.arange(GX, dtype=jnp.float32)
    grid_y = jnp.arange(GY, dtype=jnp.float32)
    phase = 2.0 * math.pi * (freq_x[:, None, None] * grid_x[None, :, None] / GX + freq_y[:, None, None] * grid_y[None, None, :] / GY)
    scale_base = 1.0 / math.sqrt(gsize)
    base_real = jnp.cos(phase) * scale_base
    base_imag = jnp.sin(phase) * scale_base
    mixing = 0.08 * jax.random.uniform(key_mix, (NKX, NKY, 2, NSTORE, NSTORE), jnp.float32, -1.0, 1.0)
    mix_real = jnp.eye(NSTORE, dtype=jnp.float32) + mixing[:, :, 0]
    mix_imag = mixing[:, :, 1]
    field_real = jnp.einsum('abmn,mxy->abnxy', mix_real, base_real) - jnp.einsum('abmn,mxy->abnxy', mix_imag, base_imag)
    field_imag = jnp.einsum('abmn,mxy->abnxy', mix_real, base_imag) + jnp.einsum('abmn,mxy->abnxy', mix_imag, base_real)
    noise = 0.3 * scale_base * jax.random.normal(key_noise, (NKX, NKY, 2, NSTORE, GX, GY), jnp.float32)
    return (jnp.stack([field_real, field_imag], axis=2) + noise).astype(jnp.bfloat16)


def draw_bands(key, part):
    return jax.random.permutation(jax.random.fold_in(key, 23), NSTORE)[:NBAND].astype(jnp.int32)


def touch_ends(values, rng, least, high):
    index_at = [jax.random.randint(jax.random.fold_in(rng, axis), (), 0, length) for axis, length in enumerate(values.shape)]
    main_axis = values.shape.index(max(values.shape))
    neighbour = index_at[:main_axis] + [(index_at[main_axis] + 1) % values.shape[main_axis]] + index_at[main_axis + 1:]
    return values.at[tuple(index_at)].set(least).at[tuple(neighbour)].set(high)


def setup_inputs(seed: int = 0) -> dict:
    seeds = jax.random.split(jax.random.key(seed), 4)
    return {
        "coeffs": draw_coeffs(jax.random.fold_in(seeds[3], 71), 0),
        "bands": draw_bands(jax.random.fold_in(seeds[3], 71), 0),
        "umklapp": touch_ends(jax.random.randint(seeds[2], (2, 2), -3, 4), jax.random.fold_in(seeds[2], 1), -3, 3).astype(jnp.int32),
    }


def correlation(left_block, right_block):
    count = left_block.shape[1]
    left_rows = left_block.reshape(2 * count, -1)
    right_rows = right_block.reshape(2 * count, -1)
    square = lax.dot_general(left_rows, right_rows, (((1,), (1,)), ((), ())), preferred_element_type=jnp.float32)
    real_part = square[:count, :count] + square[count:, count:]
    imag_part = square[:count, count:] - square[count:, :count]
    return (real_part, imag_part)

def det_units(real_stack, imag_stack):
    count = real_stack.shape[1]
    places = jnp.arange(count, dtype=jnp.int32)

    def elimination(pivot_row, carry):
        work_real, work_imag, unit_real, unit_imag = carry
        pivot_real = work_real[:, pivot_row, pivot_row]
        pivot_imag = work_imag[:, pivot_row, pivot_row]
        square_mag = pivot_real * pivot_real + pivot_imag * pivot_imag
        inverse_real = pivot_real / square_mag
        inverse_imag = -pivot_imag / square_mag
        column_real = work_real[:, :, pivot_row]
        column_imag = work_imag[:, :, pivot_row]
        below = (places > pivot_row).astype(jnp.float32)[None, :]
        factor_real = (column_real * inverse_real[:, None] - column_imag * inverse_imag[:, None]) * below
        factor_imag = (column_real * inverse_imag[:, None] + column_imag * inverse_real[:, None]) * below
        row_real = work_real[:, pivot_row, :]
        row_imag = work_imag[:, pivot_row, :]
        work_real = work_real - (factor_real[:, :, None] * row_real[:, None, :] - factor_imag[:, :, None] * row_imag[:, None, :])
        work_imag = work_imag - (factor_real[:, :, None] * row_imag[:, None, :] + factor_imag[:, :, None] * row_real[:, None, :])
        magnitude = jnp.sqrt(square_mag)
        next_real = (unit_real * pivot_real - unit_imag * pivot_imag) / magnitude
        next_imag = (unit_real * pivot_imag + unit_imag * pivot_real) / magnitude
        return (work_real, work_imag, next_real, next_imag)
    batch = real_stack.shape[0]
    start = (real_stack, imag_stack, jnp.ones((batch,), jnp.float32), jnp.zeros((batch,), jnp.float32))
    result = lax.fori_loop(0, count, elimination, start)
    return jnp.stack([result[2], result[3]], axis=-1)

def rolled(block, offset):
    return jnp.roll(block, (offset[0], offset[1]), axis=(2, 3))

def times(first, second):
    return jnp.stack([first[..., 0] * second[..., 0] - first[..., 1] * second[..., 1], first[..., 0] * second[..., 1] + first[..., 1] * second[..., 0]], axis=-1)

def conjugate(value):
    return jnp.stack([value[..., 0], -value[..., 1]], axis=-1)

def reference(coeffs, bands, umklapp):

    def one_point(flat):
        row = flat // NKY
        column = flat % NKY
        next_row = (row + 1) % NKX
        next_column = (column + 1) % NKY
        own_block = jnp.take(coeffs[row, column], bands, axis=1)
        right_block = jnp.take(coeffs[next_row, column], bands, axis=1)
        upper_block = jnp.take(coeffs[row, next_column], bands, axis=1)
        corner_block = jnp.take(coeffs[next_row, next_column], bands, axis=1)
        shift_x = jnp.where(row == NKX - 1, umklapp[0], jnp.zeros((2,), jnp.int32))
        shift_y = jnp.where(column == NKY - 1, umklapp[1], jnp.zeros((2,), jnp.int32))
        first_real, first_imag = correlation(own_block, rolled(right_block, shift_x))
        second_real, second_imag = correlation(own_block, rolled(upper_block, shift_y))
        third_real, third_imag = correlation(own_block, rolled(corner_block, shift_x + shift_y))
        real_stack = jnp.stack([first_real, second_real, third_real])
        imag_stack = jnp.stack([first_imag, second_imag, third_imag])
        return det_units(real_stack, imag_stack)
    links = lax.map(one_point, jnp.arange(NKX * NKY, dtype=jnp.int32)).reshape(NKX, NKY, 3, 2)
    along_x = links[:, :, 0]
    along_y = links[:, :, 1]
    along_d = links[:, :, 2]
    y_next = jnp.roll(along_y, -1, axis=0)
    x_next = jnp.roll(along_x, -1, axis=1)
    first = times(times(along_x, y_next), conjugate(along_d))
    second = times(times(along_d, conjugate(x_next)), conjugate(along_y))
    flux = jnp.stack([jnp.arctan2(first[..., 1], first[..., 0]), jnp.arctan2(second[..., 1], second[..., 0])], axis=-1)
    return (flux, links)
```

```python
import functools

import jax
import jax.numpy as jnp
from jax import lax
from jax.experimental import pallas as pl
from jax.experimental.pallas import tpu as pltpu
from jax.sharding import PartitionSpec as P

MESH = pl.DeviceIdType.MESH
NT = (((1,), (1,)), ((), ()))
PREP = 8
PIECE = 8


def kernel(
    coeffs, bands_far, umklapp_far, out,
    bands, umklapp, first, rest, plain, local, shifted, upper, left, early, late, early_x, early_d, late_x,
    load_sem, z_send, z_recv, x_send, x_recv, mail_send, mail_recv,
):
    rows, count, cols = plain.shape
    nband = bands.shape[0]
    pieces = rows // PIECE
    nx, ny = lax.axis_size("kx"), lax.axis_size("ky")
    i, j = lax.axis_index("kx"), lax.axis_index("ky")
    i_next, i_prev = lax.rem(i + 1, nx), lax.rem(i + nx - 1, nx)
    j_next, j_prev = lax.rem(j + 1, ny), lax.rem(j + ny - 1, ny)

    load_first = pltpu.make_async_copy(
        coeffs.at[:, :, pl.ds(0, PREP)], first, load_sem.at[0]
    )
    load_rest = pltpu.make_async_copy(
        coeffs.at[:, :, pl.ds(PREP, rows - PREP)], rest, load_sem.at[1]
    )
    load_bands = pltpu.make_async_copy(bands_far, bands, load_sem.at[2])
    load_umklapp = pltpu.make_async_copy(umklapp_far, umklapp, load_sem.at[3])
    load_bands.start()
    load_first.start()
    load_umklapp.start()
    load_rest.start()

    barrier = pltpu.get_barrier_semaphore()
    partners = [(i, j_prev), (i, j_next), (i_prev, j), (i_next, j)]
    for partner in partners:
        pl.semaphore_signal(barrier, inc=1, device_id=partner, device_id_type=MESH)

    def z_copy(piece):
        span = pl.ds(piece * PIECE, PIECE)
        return pltpu.make_async_remote_copy(
            src_ref=plain.at[span], dst_ref=upper.at[span],
            send_sem=z_send.at[0], recv_sem=z_recv.at[piece],
            device_id=(i, j_prev), device_id_type=MESH,
        )

    def x_copy(piece):
        span = pl.ds(piece * PIECE, PIECE)
        return pltpu.make_async_remote_copy(
            src_ref=shifted.at[span], dst_ref=left.at[span],
            send_sem=x_send.at[0], recv_sem=x_recv.at[piece],
            device_id=(i_next, j), device_id_type=MESH,
        )

    def gather(source, start, target):
        picked = [
            source[part, bands[band], pl.ds(start, PREP), :]
            for part in range(2)
            for band in range(nband)
        ]
        block = jnp.stack(picked).astype(jnp.float32)
        plain[pl.ds(target, PREP)] = jnp.swapaxes(block, 0, 1).astype(jnp.bfloat16)

    def send_plain(step):
        for k in range(PREP // PIECE):
            z_copy(step * (PREP // PIECE) + k).start()

    load_bands.wait()
    load_first.wait()
    gather(first, 0, 0)
    pl.semaphore_wait(barrier, len(partners))
    send_plain(0)
    load_rest.wait()
    load_umklapp.wait()

    def gather_step(step, _):
        gather(rest, pl.multiple_of((step - 1) * PREP, PREP), step * PREP)
        send_plain(step)
        return 0

    lax.fori_loop(1, rows // PREP, gather_step, 0)

    off_x = [jnp.where(i == nx - 1, umklapp[0, c], 0) for c in range(2)]
    off_y = [jnp.where(j == ny - 1, umklapp[1, c], 0) for c in range(2)]
    distance = lax.broadcasted_iota(jnp.int32, (cols, cols), 0) - lax.broadcasted_iota(
        jnp.int32, (cols, cols), 1
    )

    def mover(shift):
        far = distance - shift
        hit = (far == 0) | (far == cols) | (far == -cols)
        return jnp.where(hit, 1.0, 0.0).astype(jnp.bfloat16)

    def roll_group(target, start, shift, move):
        block = jnp.concatenate(
            [plain[lax.rem(start + k + shift + rows, rows)] for k in range(4)], axis=0
        )
        moved = jnp.dot(block, move, preferred_element_type=jnp.float32).astype(jnp.bfloat16)
        target[pl.ds(start, 4)] = moved.reshape(4, count, cols)

    move_far = mover(off_x[1] + off_y[1])

    def shift_step(piece, _):
        for k in range(PIECE // 4):
            roll_group(shifted, piece * PIECE + 4 * k, off_x[0] + off_y[0], move_far)
        x_copy(piece).start()
        return 0

    lax.fori_loop(0, pieces, shift_step, 0)
    move_near = mover(off_y[1])

    def local_step(step, _):
        roll_group(local, step * 4, off_y[0], move_near)
        return 0

    lax.fori_loop(0, rows // 4, local_step, 0)

    def left_step(piece, total):
        x_copy(piece).wait_recv()
        for k in range(PIECE):
            row = piece * PIECE + k
            total = total + lax.dot_general(
                left[row], local[row], NT, preferred_element_type=jnp.float32
            )
        return total

    width = 2 * count
    back = width - nband

    def parted(square):
        wide = jnp.concatenate([square, square], axis=1)
        upper_half, lower_half = wide[:nband], wide[nband:]
        return (
            upper_half + pltpu.roll(lower_half, back, 1),
            pltpu.roll(upper_half, back, 1) - lower_half,
        )

    def mail_to(box, slot, index, device):
        return pltpu.make_async_remote_copy(
            src_ref=box, dst_ref=slot, send_sem=mail_send.at[index], recv_sem=mail_recv.at[index],
            device_id=device, device_id_type=MESH,
        )

    total_x = lax.fori_loop(0, pieces, left_step, jnp.zeros((count, count), jnp.float32))
    unit_re, unit_im = det_units(*parted(total_x))
    early[0:1] = unit_re
    early[1:2] = unit_im
    early_to_x = mail_to(early, early_x, 1, (i_prev, j))
    early_to_x.start()
    early_to_x.wait_recv()
    early_to_d = mail_to(early_x, early_d, 0, (i, j_prev))
    early_to_d.start()

    def upper_step(piece, total):
        z_copy(piece).wait_recv()
        for k in range(PIECE):
            row = piece * PIECE + k
            lhs = jnp.concatenate([left[row], local[row]], axis=0)
            total = total + lax.dot_general(lhs, upper[row], NT, preferred_element_type=jnp.float32)
        return total

    total = lax.fori_loop(0, pieces, upper_step, jnp.zeros((2 * count, count), jnp.float32))
    lane = lax.broadcasted_iota(jnp.int32, (nband, width), 1)
    d_re, d_im = parted(total[:count])
    y_re, y_im = parted(total[count:])
    unit_re, unit_im = det_units(
        jnp.where(lane < count, d_re, y_re), jnp.where(lane < count, d_im, y_im)
    )
    late[0:1] = unit_re
    late[1:2] = unit_im
    late_to_x = mail_to(late, late_x, 2, (i_prev, j))
    late_to_x.start()

    pltpu.make_async_remote_copy(
        src_ref=plain, dst_ref=upper, send_sem=z_send.at[0], recv_sem=z_recv.at[0],
        device_id=(i, j_prev), device_id_type=MESH,
    ).wait_send()
    pltpu.make_async_remote_copy(
        src_ref=shifted, dst_ref=left, send_sem=x_send.at[0], recv_sem=x_recv.at[0],
        device_id=(i_next, j), device_id_type=MESH,
    ).wait_send()
    early_to_x.wait_send()
    early_to_d.wait()
    along_y = (pltpu.roll(unit_re, count, 1), pltpu.roll(unit_im, count, 1))
    along_x = (early_x[0:1], early_x[1:2])
    x_next = (early_d[0:1], early_d[1:2])
    rest_of_second = times(conjugate(x_next), conjugate(along_y))
    late_to_x.wait()
    late_re, late_im = late_x[0:1], late_x[1:2]
    along_d = (late_re, late_im)
    y_next = (pltpu.roll(late_re, count, 1), pltpu.roll(late_im, count, 1))
    one = times(times(along_x, y_next), conjugate(along_d))
    two = times(along_d, rest_of_second)
    at_zero = lax.broadcasted_iota(jnp.int32, (1, width), 1) == 0
    angle = jnp.arctan2(jnp.where(at_zero, one[1], two[1]), jnp.where(at_zero, one[0], two[0]))
    spot = lax.broadcasted_iota(jnp.int32, (1, width), 1)

    def placed(part):
        return jnp.where(
            spot == 0, along_x[part], jnp.where(spot == 1, along_y[part], along_d[part])
        )

    out[0:1] = angle
    out[1:2] = placed(0)
    out[2:3] = placed(1)
    out[3:8] = jnp.zeros((5, width), jnp.float32)


def split(found, flux, links):
    flux[0] = found[0:1, :2]
    links[0, 0] = found[1:3, :3]


def det_units(work_re, work_im):
    nband, width = work_re.shape
    tiles = nband // 8
    re = [work_re[8 * g : 8 * g + 8] for g in range(tiles)]
    im = [work_im[8 * g : 8 * g + 8] for g in range(tiles)]
    lane8 = lax.broadcasted_iota(jnp.int32, (8, width), 1)
    group_start = lane8 - lax.rem(lane8, nband)
    unit = (jnp.ones((1, width), jnp.float32), jnp.zeros((1, width), jnp.float32))
    for g0 in range(tiles):
        live = range(g0, tiles)
        cols = []
        for m in range(8):
            place = group_start + (8 * g0 + m)
            cols.append({
                g: (
                    jnp.take_along_axis(re[g], place, axis=1),
                    jnp.take_along_axis(im[g], place, axis=1),
                )
                for g in live
            })
        for m in range(8):
            pr, pi = cols[m][g0][0][m : m + 1], cols[m][g0][1][m : m + 1]
            square = pr * pr + pi * pi
            scale = lax.rsqrt(square)
            unit = times(unit, (pr * scale, pi * scale))
            if 8 * g0 + m == nband - 1:
                break
            inverse = 1.0 / square
            against = {g: times(cols[m][g], (pr, -pi)) for g in live}
            factor = {g: (against[g][0] * inverse, against[g][1] * inverse) for g in live}
            for n in range(m + 1, 8):
                row = (cols[n][g0][0][m : m + 1], cols[n][g0][1][m : m + 1])
                for g in live:
                    if n == m + 1 and g == g0:
                        less = times(against[g], row)
                        less = (less[0] * inverse, less[1] * inverse)
                    else:
                        less = times(factor[g], row)
                    cols[n][g] = (cols[n][g][0] - less[0], cols[n][g][1] - less[1])
            if g0 + 1 < tiles:
                row = (re[g0][m : m + 1], im[g0][m : m + 1])
                for g in live:
                    less = times(factor[g], row)
                    re[g] = re[g] - less[0]
                    im[g] = im[g] - less[1]
    size = 1.0 / jnp.sqrt(unit[0] * unit[0] + unit[1] * unit[1])
    return unit[0] * size, unit[1] * size


def times(first, second):
    return (
        first[0] * second[0] - first[1] * second[1],
        first[0] * second[1] + first[1] * second[0],
    )


def conjugate(value):
    return (value[0], -value[1])


def per_device(coeffs, bands, umklapp):
    block = coeffs[0, 0]
    rows, cols = block.shape[2], block.shape[3]
    nstore, nband = block.shape[1], bands.shape[0]
    count = 2 * nband
    pieces = rows // PIECE
    side = pltpu.VMEM((rows, count, cols), jnp.bfloat16)
    tile = pltpu.VMEM((8, 2 * count), jnp.float32)
    found = pl.pallas_call(
        kernel,
        out_shape=jax.ShapeDtypeStruct((8, 2 * count), jnp.float32),
        in_specs=[pl.BlockSpec(memory_space=pl.ANY)] * 3,
        out_specs=pl.BlockSpec(memory_space=pltpu.VMEM),
        scratch_shapes=[
            pltpu.SMEM(bands.shape, jnp.int32),
            pltpu.SMEM(umklapp.shape, jnp.int32),
            pltpu.VMEM((2, nstore, PREP, cols), jnp.bfloat16),
            pltpu.VMEM((2, nstore, rows - PREP, cols), jnp.bfloat16),
            side, side, side, side, side,
            tile, tile, tile, tile, tile,
            pltpu.SemaphoreType.DMA((4,)),
            pltpu.SemaphoreType.DMA((1,)),
            pltpu.SemaphoreType.DMA((pieces,)),
            pltpu.SemaphoreType.DMA((1,)),
            pltpu.SemaphoreType.DMA((pieces,)),
            pltpu.SemaphoreType.DMA((3,)),
            pltpu.SemaphoreType.DMA((3,)),
        ],
        compiler_params=pltpu.CompilerParams(
            collective_id=0, has_side_effects=True, vmem_limit_bytes=63 * 1024 * 1024
        ),
    )(block, bands, umklapp)
    flux, links = pl.pallas_call(
        split,
        out_shape=(
            jax.ShapeDtypeStruct((1, 1, 2), jnp.float32),
            jax.ShapeDtypeStruct((1, 1, 2, 3), jnp.float32),
        ),
        in_specs=[pl.BlockSpec(memory_space=pltpu.VMEM)],
        out_specs=(
            pl.BlockSpec(memory_space=pltpu.VMEM),
            pl.BlockSpec(memory_space=pltpu.VMEM),
        ),
    )(found)
    return (flux, jnp.swapaxes(links, 2, 3))


def solution(mesh):
    in_specs = (P("kx", "ky", None, None, None, None), P(), P())
    out_specs = (P("kx", "ky", None), P("kx", "ky", None, None))
    return jax.shard_map(
        per_device, mesh=mesh, in_specs=in_specs, out_specs=out_specs, check_vma=False
    )
```

```python
import functools

import jax
import jax.numpy as jnp
from jax import lax
from jax.experimental import pallas as pl
from jax.experimental.pallas import tpu as pltpu
from jax.sharding import PartitionSpec as P

MESH = pl.DeviceIdType.MESH
NT = (((1,), (1,)), ((), ()))
PREP = 8
PIECE = 8


def kernel(
    coeffs, bands_far, umklapp_far, out,
    bands, umklapp, first, rest, plain, local, shifted, upper, left, early, late, early_x, early_d, late_x,
    load_sem, z_send, z_recv, x_send, x_recv, mail_send, mail_recv,
):
    rows, count, cols = plain.shape
    nband = bands.shape[0]
    pieces = rows // PIECE
    nx, ny = lax.axis_size("kx"), lax.axis_size("ky")
    i, j = lax.axis_index("kx"), lax.axis_index("ky")
    i_next, i_prev = lax.rem(i + 1, nx), lax.rem(i + nx - 1, nx)
    j_next, j_prev = lax.rem(j + 1, ny), lax.rem(j + ny - 1, ny)

    load_first = pltpu.make_async_copy(
        coeffs.at[:, :, pl.ds(0, PREP)], first, load_sem.at[0]
    )
    load_rest = pltpu.make_async_copy(
        coeffs.at[:, :, pl.ds(PREP, rows - PREP)], rest, load_sem.at[1]
    )
    load_bands = pltpu.make_async_copy(bands_far, bands, load_sem.at[2])
    load_umklapp = pltpu.make_async_copy(umklapp_far, umklapp, load_sem.at[3])
    load_bands.start()
    load_first.start()
    load_umklapp.start()
    load_rest.start()

    barrier = pltpu.get_barrier_semaphore()
    partners = [(i, j_prev), (i, j_next), (i_prev, j), (i_next, j)]
    for partner in partners:
        pl.semaphore_signal(barrier, inc=1, device_id=partner, device_id_type=MESH)

    def z_copy(piece):
        span = pl.ds(piece * PIECE, PIECE)
        return pltpu.make_async_remote_copy(
            src_ref=plain.at[span], dst_ref=upper.at[span],
            send_sem=z_send.at[0], recv_sem=z_recv.at[piece],
            device_id=(i, j_prev), device_id_type=MESH,
        )

    def x_copy(piece):
        span = pl.ds(piece * PIECE, PIECE)
        return pltpu.make_async_remote_copy(
            src_ref=shifted.at[span], dst_ref=left.at[span],
            send_sem=x_send.at[0], recv_sem=x_recv.at[piece],
            device_id=(i_next, j), device_id_type=MESH,
        )

    def gather(source, start, target):
        picked = [
            source[part, bands[band], pl.ds(start, PREP), :]
            for part in range(2)
            for band in range(nband)
        ]
        block = jnp.stack(picked).astype(jnp.float32)
        plain[pl.ds(target, PREP)] = jnp.swapaxes(block, 0, 1).astype(jnp.bfloat16)

    def send_plain(step):
        for k in range(PREP // PIECE):
            z_copy(step * (PREP // PIECE) + k).start()

    load_bands.wait()
    load_first.wait()
    gather(first, 0, 0)
    pl.semaphore_wait(barrier, len(partners))
    send_plain(0)
    load_rest.wait()
    load_umklapp.wait()

    def gather_step(step, _):
        gather(rest, pl.multiple_of((step - 1) * PREP, PREP), step * PREP)
        send_plain(step)
        return 0

    lax.fori_loop(1, rows // PREP, gather_step, 0)

    off_x = [jnp.where(i == nx - 1, umklapp[0, c], 0) for c in range(2)]
    off_y = [jnp.where(j == ny - 1, umklapp[1, c], 0) for c in range(2)]
    distance = lax.broadcasted_iota(jnp.int32, (cols, cols), 0) - lax.broadcasted_iota(
        jnp.int32, (cols, cols), 1
    )

    def mover(shift):
        far = distance - shift
        hit = (far == 0) | (far == cols) | (far == -cols)
        return jnp.where(hit, 1.0, 0.0).astype(jnp.bfloat16)

    def roll_group(target, start, shift, move):
        block = jnp.concatenate(
            [plain[lax.rem(start + k + shift + rows, rows)] for k in range(4)], axis=0
        )
        moved = jnp.dot(block, move, preferred_element_type=jnp.float32).astype(jnp.bfloat16)
        target[pl.ds(start, 4)] = moved.reshape(4, count, cols)

    move_far = mover(off_x[1] + off_y[1])

    def shift_step(piece, _):
        for k in range(PIECE // 4):
            roll_group(shifted, piece * PIECE + 4 * k, off_x[0] + off_y[0], move_far)
        x_copy(piece).start()
        return 0

    lax.fori_loop(0, pieces, shift_step, 0)
    move_near = mover(off_y[1])

    def local_step(step, _):
        roll_group(local, step * 4, off_y[0], move_near)
        return 0

    lax.fori_loop(0, rows // 4, local_step, 0)

    def left_step(piece, total):
        x_copy(piece).wait_recv()
        for k in range(PIECE):
            row = piece * PIECE + k
            total = total + lax.dot_general(
                left[row], local[row], NT, preferred_element_type=jnp.float32
            )
        return total

    width = 2 * count
    back = width - nband

    def parted(square):
        wide = jnp.concatenate([square, square], axis=1)
        upper_half, lower_half = wide[:nband], wide[nband:]
        return (
            upper_half + pltpu.roll(lower_half, back, 1),
            pltpu.roll(upper_half, back, 1) - lower_half,
        )

    def mail_to(box, slot, index, device):
        return pltpu.make_async_remote_copy(
            src_ref=box, dst_ref=slot, send_sem=mail_send.at[index], recv_sem=mail_recv.at[index],
            device_id=device, device_id_type=MESH,
        )

    total_x = lax.fori_loop(0, pieces, left_step, jnp.zeros((count, count), jnp.float32))
    unit_re, unit_im = det_units(*parted(total_x))
    early[0:1] = unit_re
    early[1:2] = unit_im
    early_to_x = mail_to(early, early_x, 1, (i_prev, j))
    early_to_x.start()
    early_to_x.wait_recv()
    early_to_d = mail_to(early_x, early_d, 0, (i, j_prev))
    early_to_d.start()

    def upper_step(piece, total):
        z_copy(piece).wait_recv()
        for k in range(PIECE):
            row = piece * PIECE + k
            lhs = jnp.concatenate([left[row], local[row]], axis=0)
            total = total + lax.dot_general(lhs, upper[row], NT, preferred_element_type=jnp.float32)
        return total

    total = lax.fori_loop(0, pieces, upper_step, jnp.zeros((2 * count, count), jnp.float32))
    lane = lax.broadcasted_iota(jnp.int32, (nband, width), 1)
    d_re, d_im = parted(total[:count])
    y_re, y_im = parted(total[count:])
    unit_re, unit_im = det_units(
        jnp.where(lane < count, d_re, y_re), jnp.where(lane < count, d_im, y_im)
    )
    late[0:1] = unit_re
    late[1:2] = unit_im
    late_to_x = mail_to(late, late_x, 2, (i_prev, j))
    late_to_x.start()

    pltpu.make_async_remote_copy(
        src_ref=plain, dst_ref=upper, send_sem=z_send.at[0], recv_sem=z_recv.at[0],
        device_id=(i, j_prev), device_id_type=MESH,
    ).wait_send()
    pltpu.make_async_remote_copy(
        src_ref=shifted, dst_ref=left, send_sem=x_send.at[0], recv_sem=x_recv.at[0],
        device_id=(i_next, j), device_id_type=MESH,
    ).wait_send()
    early_to_x.wait_send()
    early_to_d.wait()
    along_y = (pltpu.roll(unit_re, count, 1), pltpu.roll(unit_im, count, 1))
    along_x = (early_x[0:1], early_x[1:2])
    x_next = (early_d[0:1], early_d[1:2])
    rest_of_second = times(conjugate(x_next), conjugate(along_y))
    late_to_x.wait()
    late_re, late_im = late_x[0:1], late_x[1:2]
    along_d = (late_re, late_im)
    y_next = (pltpu.roll(late_re, count, 1), pltpu.roll(late_im, count, 1))
    one = times(times(along_x, y_next), conjugate(along_d))
    two = times(along_d, rest_of_second)
    at_zero = lax.broadcasted_iota(jnp.int32, (1, width), 1) == 0
    angle = jnp.arctan2(jnp.where(at_zero, one[1], two[1]), jnp.where(at_zero, one[0], two[0]))
    spot = lax.broadcasted_iota(jnp.int32, (1, width), 1)

    def placed(part):
        return jnp.where(
            spot == 0, along_x[part], jnp.where(spot == 1, along_y[part], along_d[part])
        )

    out[0:1] = angle
    out[1:2] = placed(0)
    out[2:3] = placed(1)
    out[3:8] = jnp.zeros((5, width), jnp.float32)


def split(found, flux, links):
    flux[0] = found[0:1, :2]
    links[0, 0] = found[1:3, :3]


def det_units(work_re, work_im):
    nband, width = work_re.shape
    tiles = nband // 8
    re = [work_re[8 * g : 8 * g + 8] for g in range(tiles)]
    im = [work_im[8 * g : 8 * g + 8] for g in range(tiles)]
    lane8 = lax.broadcasted_iota(jnp.int32, (8, width), 1)
    group_start = lane8 - lax.rem(lane8, nband)
    unit = (jnp.ones((1, width), jnp.float32), jnp.zeros((1, width), jnp.float32))
    for g0 in range(tiles):
        live = range(g0, tiles)
        cols = []
        for m in range(8):
            place = group_start + (8 * g0 + m)
            cols.append({
                g: (
                    jnp.take_along_axis(re[g], place, axis=1),
                    jnp.take_along_axis(im[g], place, axis=1),
                )
                for g in live
            })
        for m in range(8):
            pr, pi = cols[m][g0][0][m : m + 1], cols[m][g0][1][m : m + 1]
            square = pr * pr + pi * pi
            scale = lax.rsqrt(square)
            unit = times(unit, (pr * scale, pi * scale))
            if 8 * g0 + m == nband - 1:
                break
            inverse = 1.0 / square
            against = {g: times(cols[m][g], (pr, -pi)) for g in live}
            factor = {g: (against[g][0] * inverse, against[g][1] * inverse) for g in live}
            for n in range(m + 1, 8):
                row = (cols[n][g0][0][m : m + 1], cols[n][g0][1][m : m + 1])
                for g in live:
                    if n == m + 1 and g == g0:
                        less = times(against[g], row)
                        less = (less[0] * inverse, less[1] * inverse)
                    else:
                        less = times(factor[g], row)
                    cols[n][g] = (cols[n][g][0] - less[0], cols[n][g][1] - less[1])
            if g0 + 1 < tiles:
                row = (re[g0][m : m + 1], im[g0][m : m + 1])
                for g in live:
                    less = times(factor[g], row)
                    re[g] = re[g] - less[0]
                    im[g] = im[g] - less[1]
    size = 1.0 / jnp.sqrt(unit[0] * unit[0] + unit[1] * unit[1])
    return unit[0] * size, unit[1] * size


def times(first, second):
    return (
        first[0] * second[0] - first[1] * second[1],
        first[0] * second[1] + first[1] * second[0],
    )


def conjugate(value):
    return (value[0], -value[1])


def per_device(coeffs, bands, umklapp):
    block = coeffs[0, 0]
    rows, cols = block.shape[2], block.shape[3]
    nstore, nband = block.shape[1], bands.shape[0]
    count = 2 * nband
    pieces = rows // PIECE
    side = pltpu.VMEM((rows, count, cols), jnp.bfloat16)
    tile = pltpu.VMEM((8, 2 * count), jnp.float32)
    found = pl.pallas_call(
        kernel,
        out_shape=pltpu.VMEM((8, 2 * count), jnp.float32),
        in_specs=[pl.BlockSpec(memory_space=pl.ANY)] * 3,
        out_specs=pl.BlockSpec(memory_space=pltpu.VMEM),
        scratch_shapes=[
            pltpu.SMEM(bands.shape, jnp.int32),
            pltpu.SMEM(umklapp.shape, jnp.int32),
            pltpu.VMEM((2, nstore, PREP, cols), jnp.bfloat16),
            pltpu.VMEM((2, nstore, rows - PREP, cols), jnp.bfloat16),
            side, side, side, side, side,
            tile, tile, tile, tile, tile,
            pltpu.SemaphoreType.DMA((4,)),
            pltpu.SemaphoreType.DMA((1,)),
            pltpu.SemaphoreType.DMA((pieces,)),
            pltpu.SemaphoreType.DMA((1,)),
            pltpu.SemaphoreType.DMA((pieces,)),
            pltpu.SemaphoreType.DMA((3,)),
            pltpu.SemaphoreType.DMA((3,)),
        ],
        compiler_params=pltpu.CompilerParams(
            collective_id=0, has_side_effects=True, vmem_limit_bytes=56 * 1024 * 1024
        ),
    )(block, bands, umklapp)
    flux, links = pl.pallas_call(
        split,
        out_shape=(
            jax.ShapeDtypeStruct((1, 1, 2), jnp.float32),
            jax.ShapeDtypeStruct((1, 1, 2, 3), jnp.float32),
        ),
        in_specs=[pl.BlockSpec(memory_space=pltpu.VMEM)],
        out_specs=(
            pl.BlockSpec(memory_space=pltpu.VMEM),
            pl.BlockSpec(memory_space=pltpu.VMEM),
        ),
        compiler_params=pltpu.CompilerParams(vmem_limit_bytes=1024 * 1024),
    )(found)
    return (flux, jnp.swapaxes(links, 2, 3))


def solution(mesh):
    in_specs = (P("kx", "ky", None, None, None, None), P(), P())
    out_specs = (P("kx", "ky", None), P("kx", "ky", None, None))
    return jax.shard_map(
        per_device, mesh=mesh, in_specs=in_specs, out_specs=out_specs, check_vma=False
    )
```

```python
import functools

import jax
import jax.numpy as jnp
from jax import lax
from jax.experimental import pallas as pl
from jax.experimental.pallas import tpu as pltpu
from jax.sharding import PartitionSpec as P

MESH = pl.DeviceIdType.MESH
NT = (((1,), (1,)), ((), ()))
PREP = 8
PIECE = 8


def kernel(
    coeffs, bands_far, umklapp_far, out,
    bands, umklapp, first, rest, plain, local, shifted, upper, left, early, late, early_x, early_d, late_x,
    load_sem, z_send, z_recv, x_send, x_recv, mail_send, mail_recv,
):
    rows, count, cols = plain.shape
    nband = bands.shape[0]
    pieces = rows // PIECE
    nx, ny = lax.axis_size("kx"), lax.axis_size("ky")
    i, j = lax.axis_index("kx"), lax.axis_index("ky")
    i_next, i_prev = lax.rem(i + 1, nx), lax.rem(i + nx - 1, nx)
    j_next, j_prev = lax.rem(j + 1, ny), lax.rem(j + ny - 1, ny)

    load_first = pltpu.make_async_copy(
        coeffs.at[:, :, pl.ds(0, PREP)], first, load_sem.at[0]
    )
    load_rest = pltpu.make_async_copy(
        coeffs.at[:, :, pl.ds(PREP, rows - PREP)], rest, load_sem.at[1]
    )
    load_bands = pltpu.make_async_copy(bands_far, bands, load_sem.at[2])
    load_umklapp = pltpu.make_async_copy(umklapp_far, umklapp, load_sem.at[3])
    load_bands.start()
    load_first.start()
    load_umklapp.start()
    load_rest.start()

    barrier = pltpu.get_barrier_semaphore()
    partners = [(i, j_prev), (i, j_next), (i_prev, j), (i_next, j)]
    for partner in partners:
        pl.semaphore_signal(barrier, inc=1, device_id=partner, device_id_type=MESH)

    def z_copy(piece):
        span = pl.ds(piece * PIECE, PIECE)
        return pltpu.make_async_remote_copy(
            src_ref=plain.at[span], dst_ref=upper.at[span],
            send_sem=z_send.at[0], recv_sem=z_recv.at[piece],
            device_id=(i, j_prev), device_id_type=MESH,
        )

    def x_copy(piece):
        span = pl.ds(piece * PIECE, PIECE)
        return pltpu.make_async_remote_copy(
            src_ref=shifted.at[span], dst_ref=left.at[span],
            send_sem=x_send.at[0], recv_sem=x_recv.at[piece],
            device_id=(i_next, j), device_id_type=MESH,
        )

    def gather(source, start, target):
        picked = [
            source[part, bands[band], pl.ds(start, PREP), :]
            for part in range(2)
            for band in range(nband)
        ]
        block = jnp.stack(picked).astype(jnp.float32)
        plain[pl.ds(target, PREP)] = jnp.swapaxes(block, 0, 1).astype(jnp.bfloat16)

    at_once = jnp.where(lax.rem(i, 2) == 0, pieces, 1)

    def send_plain(piece):
        @pl.when(piece < at_once)
        def _():
            z_copy(piece).start()

    def send_late(piece, _):
        z_copy(piece).start()
        return 0

    load_bands.wait()
    load_first.wait()
    gather(first, 0, 0)
    pl.semaphore_wait(barrier, len(partners))
    send_plain(0)
    load_rest.wait()
    load_umklapp.wait()

    def gather_step(step, _):
        gather(rest, pl.multiple_of((step - 1) * PREP, PREP), step * PREP)
        send_plain(step)
        return 0

    lax.fori_loop(1, rows // PREP, gather_step, 0)

    off_x = [jnp.where(i == nx - 1, umklapp[0, c], 0) for c in range(2)]
    off_y = [jnp.where(j == ny - 1, umklapp[1, c], 0) for c in range(2)]
    distance = lax.broadcasted_iota(jnp.int32, (cols, cols), 0) - lax.broadcasted_iota(
        jnp.int32, (cols, cols), 1
    )

    def mover(shift):
        far = distance - shift
        hit = (far == 0) | (far == cols) | (far == -cols)
        return jnp.where(hit, 1.0, 0.0).astype(jnp.bfloat16)

    def roll_group(target, start, shift, move):
        block = jnp.concatenate(
            [plain[lax.rem(start + k + shift + rows, rows)] for k in range(4)], axis=0
        )
        moved = jnp.dot(block, move, preferred_element_type=jnp.float32).astype(jnp.bfloat16)
        target[pl.ds(start, 4)] = moved.reshape(4, count, cols)

    move_far = mover(off_x[1] + off_y[1])

    def shift_step(piece, _):
        for k in range(PIECE // 4):
            roll_group(shifted, piece * PIECE + 4 * k, off_x[0] + off_y[0], move_far)
        x_copy(piece).start()
        return 0

    lax.fori_loop(0, pieces, shift_step, 0)
    move_near = mover(off_y[1])

    def local_step(step, _):
        roll_group(local, step * 4, off_y[0], move_near)
        return 0

    lax.fori_loop(0, rows // 8, local_step, 0)
    lax.fori_loop(at_once, pieces, send_late, 0)
    lax.fori_loop(rows // 8, rows // 4, local_step, 0)

    def left_step(piece, total):
        x_copy(piece).wait_recv()
        for k in range(PIECE):
            row = piece * PIECE + k
            total = total + lax.dot_general(
                left[row], local[row], NT, preferred_element_type=jnp.float32
            )
        return total

    width = 2 * count
    back = width - nband

    def parted(square):
        wide = jnp.concatenate([square, square], axis=1)
        upper_half, lower_half = wide[:nband], wide[nband:]
        return (
            upper_half + pltpu.roll(lower_half, back, 1),
            pltpu.roll(upper_half, back, 1) - lower_half,
        )

    def mail_to(box, slot, index, device):
        return pltpu.make_async_remote_copy(
            src_ref=box, dst_ref=slot, send_sem=mail_send.at[index], recv_sem=mail_recv.at[index],
            device_id=device, device_id_type=MESH,
        )

    total_x = lax.fori_loop(0, pieces, left_step, jnp.zeros((count, count), jnp.float32))
    unit_re, unit_im = det_units(*parted(total_x))
    early[0:1] = unit_re
    early[1:2] = unit_im
    early_to_x = mail_to(early, early_x, 1, (i_prev, j))
    early_to_x.start()
    early_to_x.wait_recv()
    early_to_d = mail_to(early_x, early_d, 0, (i, j_prev))
    early_to_d.start()

    def upper_step(piece, total):
        z_copy(piece).wait_recv()
        for k in range(PIECE):
            row = piece * PIECE + k
            lhs = jnp.concatenate([left[row], local[row]], axis=0)
            total = total + lax.dot_general(lhs, upper[row], NT, preferred_element_type=jnp.float32)
        return total

    total = lax.fori_loop(0, pieces, upper_step, jnp.zeros((2 * count, count), jnp.float32))
    lane = lax.broadcasted_iota(jnp.int32, (nband, width), 1)
    d_re, d_im = parted(total[:count])
    y_re, y_im = parted(total[count:])
    unit_re, unit_im = det_units(
        jnp.where(lane < count, d_re, y_re), jnp.where(lane < count, d_im, y_im)
    )
    late[0:1] = unit_re
    late[1:2] = unit_im
    late_to_x = mail_to(late, late_x, 2, (i_prev, j))
    late_to_x.start()

    pltpu.make_async_remote_copy(
        src_ref=plain, dst_ref=upper, send_sem=z_send.at[0], recv_sem=z_recv.at[0],
        device_id=(i, j_prev), device_id_type=MESH,
    ).wait_send()
    pltpu.make_async_remote_copy(
        src_ref=shifted, dst_ref=left, send_sem=x_send.at[0], recv_sem=x_recv.at[0],
        device_id=(i_next, j), device_id_type=MESH,
    ).wait_send()
    early_to_x.wait_send()
    early_to_d.wait()
    along_y = (pltpu.roll(unit_re, count, 1), pltpu.roll(unit_im, count, 1))
    along_x = (early_x[0:1], early_x[1:2])
    x_next = (early_d[0:1], early_d[1:2])
    rest_of_second = times(conjugate(x_next), conjugate(along_y))
    late_to_x.wait()
    late_re, late_im = late_x[0:1], late_x[1:2]
    along_d = (late_re, late_im)
    y_next = (pltpu.roll(late_re, count, 1), pltpu.roll(late_im, count, 1))
    one = times(times(along_x, y_next), conjugate(along_d))
    two = times(along_d, rest_of_second)
    at_zero = lax.broadcasted_iota(jnp.int32, (1, width), 1) == 0
    angle = jnp.arctan2(jnp.where(at_zero, one[1], two[1]), jnp.where(at_zero, one[0], two[0]))
    spot = lax.broadcasted_iota(jnp.int32, (1, width), 1)

    def placed(part):
        return jnp.where(
            spot == 0, along_x[part], jnp.where(spot == 1, along_y[part], along_d[part])
        )

    out[0:1] = angle
    out[1:2] = placed(0)
    out[2:3] = placed(1)
    out[3:8] = jnp.zeros((5, width), jnp.float32)


def split(found, flux, links):
    flux[0] = found[0:1, :2]
    links[0, 0] = found[1:3, :3]


def det_units(work_re, work_im):
    nband, width = work_re.shape
    tiles = nband // 8
    re = [work_re[8 * g : 8 * g + 8] for g in range(tiles)]
    im = [work_im[8 * g : 8 * g + 8] for g in range(tiles)]
    lane8 = lax.broadcasted_iota(jnp.int32, (8, width), 1)
    group_start = lane8 - lax.rem(lane8, nband)
    unit = (jnp.ones((1, width), jnp.float32), jnp.zeros((1, width), jnp.float32))
    for g0 in range(tiles):
        live = range(g0, tiles)
        cols = []
        for m in range(8):
            place = group_start + (8 * g0 + m)
            cols.append({
                g: (
                    jnp.take_along_axis(re[g], place, axis=1),
                    jnp.take_along_axis(im[g], place, axis=1),
                )
                for g in live
            })
        for m in range(8):
            pr, pi = cols[m][g0][0][m : m + 1], cols[m][g0][1][m : m + 1]
            square = pr * pr + pi * pi
            scale = lax.rsqrt(square)
            unit = times(unit, (pr * scale, pi * scale))
            if 8 * g0 + m == nband - 1:
                break
            inverse = 1.0 / square
            against = {g: times(cols[m][g], (pr, -pi)) for g in live}
            factor = {g: (against[g][0] * inverse, against[g][1] * inverse) for g in live}
            for n in range(m + 1, 8):
                row = (cols[n][g0][0][m : m + 1], cols[n][g0][1][m : m + 1])
                for g in live:
                    if n == m + 1 and g == g0:
                        less = times(against[g], row)
                        less = (less[0] * inverse, less[1] * inverse)
                    else:
                        less = times(factor[g], row)
                    cols[n][g] = (cols[n][g][0] - less[0], cols[n][g][1] - less[1])
            if g0 + 1 < tiles:
                row = (re[g0][m : m + 1], im[g0][m : m + 1])
                for g in live:
                    less = times(factor[g], row)
                    re[g] = re[g] - less[0]
                    im[g] = im[g] - less[1]
    size = 1.0 / jnp.sqrt(unit[0] * unit[0] + unit[1] * unit[1])
    return unit[0] * size, unit[1] * size


def times(first, second):
    return (
        first[0] * second[0] - first[1] * second[1],
        first[0] * second[1] + first[1] * second[0],
    )


def conjugate(value):
    return (value[0], -value[1])


def per_device(coeffs, bands, umklapp):
    block = coeffs[0, 0]
    rows, cols = block.shape[2], block.shape[3]
    nstore, nband = block.shape[1], bands.shape[0]
    count = 2 * nband
    pieces = rows // PIECE
    side = pltpu.VMEM((rows, count, cols), jnp.bfloat16)
    tile = pltpu.VMEM((8, 2 * count), jnp.float32)
    found = pl.pallas_call(
        kernel,
        out_shape=pltpu.VMEM((8, 2 * count), jnp.float32),
        in_specs=[pl.BlockSpec(memory_space=pl.ANY)] * 3,
        out_specs=pl.BlockSpec(memory_space=pltpu.VMEM),
        scratch_shapes=[
            pltpu.SMEM(bands.shape, jnp.int32),
            pltpu.SMEM(umklapp.shape, jnp.int32),
            pltpu.VMEM((2, nstore, PREP, cols), jnp.bfloat16),
            pltpu.VMEM((2, nstore, rows - PREP, cols), jnp.bfloat16),
            side, side, side, side, side,
            tile, tile, tile, tile, tile,
            pltpu.SemaphoreType.DMA((4,)),
            pltpu.SemaphoreType.DMA((1,)),
            pltpu.SemaphoreType.DMA((pieces,)),
            pltpu.SemaphoreType.DMA((1,)),
            pltpu.SemaphoreType.DMA((pieces,)),
            pltpu.SemaphoreType.DMA((3,)),
            pltpu.SemaphoreType.DMA((3,)),
        ],
        compiler_params=pltpu.CompilerParams(
            collective_id=0, has_side_effects=True, vmem_limit_bytes=56 * 1024 * 1024
        ),
    )(block, bands, umklapp)
    flux, links = pl.pallas_call(
        split,
        out_shape=(
            jax.ShapeDtypeStruct((1, 1, 2), jnp.float32),
            jax.ShapeDtypeStruct((1, 1, 2, 3), jnp.float32),
        ),
        in_specs=[pl.BlockSpec(memory_space=pltpu.VMEM)],
        out_specs=(
            pl.BlockSpec(memory_space=pltpu.VMEM),
            pl.BlockSpec(memory_space=pltpu.VMEM),
        ),
        compiler_params=pltpu.CompilerParams(vmem_limit_bytes=1024 * 1024),
    )(found)
    return (flux, jnp.swapaxes(links, 2, 3))


def solution(mesh):
    in_specs = (P("kx", "ky", None, None, None, None), P(), P())
    out_specs = (P("kx", "ky", None), P("kx", "ky", None, None))
    return jax.shard_map(
        per_device, mesh=mesh, in_specs=in_specs, out_specs=out_specs, check_vma=False
    )
```

```python
import functools

import jax
import jax.numpy as jnp
from jax import lax
from jax.experimental import pallas as pl
from jax.experimental.pallas import tpu as pltpu
from jax.sharding import PartitionSpec as P

MESH = pl.DeviceIdType.MESH
NT = (((1,), (1,)), ((), ()))
PREP = 8
PIECE = 8
LAST = 2
X_GROUP = 4
Z_GROUP = 2


def kernel(
    coeffs, bands_far, umklapp_far, out,
    bands, umklapp, first, rest, plain, local, shifted, upper, left, early, late, early_x, early_d, late_x,
    load_sem, z_send, z_recv, x_send, x_recv, mail_send, mail_recv,
):
    rows, count, cols = plain.shape
    nband = bands.shape[0]
    pieces = rows // PIECE
    parts = (PIECE - LAST, LAST)
    nx, ny = lax.axis_size("kx"), lax.axis_size("ky")
    i, j = lax.axis_index("kx"), lax.axis_index("ky")
    i_next, i_prev = lax.rem(i + 1, nx), lax.rem(i + nx - 1, nx)
    j_next, j_prev = lax.rem(j + 1, ny), lax.rem(j + ny - 1, ny)

    load_first = pltpu.make_async_copy(
        coeffs.at[:, :, pl.ds(0, PREP)], first, load_sem.at[0]
    )
    load_rest = pltpu.make_async_copy(
        coeffs.at[:, :, pl.ds(PREP, rows - PREP)], rest, load_sem.at[1]
    )
    load_bands = pltpu.make_async_copy(bands_far, bands, load_sem.at[2])
    load_umklapp = pltpu.make_async_copy(umklapp_far, umklapp, load_sem.at[3])
    load_bands.start()
    load_first.start()
    load_umklapp.start()
    load_rest.start()

    barrier = pltpu.get_barrier_semaphore()
    partners = [(i, j_next), (i_prev, j)]
    for partner in partners:
        pl.semaphore_signal(barrier, inc=1, device_id=partner, device_id_type=MESH)

    def z_copy(piece):
        span = pl.ds(piece * PIECE, PIECE)
        return pltpu.make_async_remote_copy(
            src_ref=plain.at[span], dst_ref=upper.at[span],
            send_sem=z_send.at[0], recv_sem=z_recv.at[2 + piece // Z_GROUP],
            device_id=(i, j_prev), device_id_type=MESH,
        )

    def z_group(piece, size):
        span = pl.ds(piece * PIECE, size * PIECE)
        return pltpu.make_async_remote_copy(
            src_ref=plain.at[span], dst_ref=upper.at[span],
            send_sem=z_send.at[0], recv_sem=z_recv.at[2 + piece // Z_GROUP],
            device_id=(i, j_prev), device_id_type=MESH,
        )

    def x_group(piece):
        span = pl.ds(piece * PIECE, X_GROUP * PIECE)
        return pltpu.make_async_remote_copy(
            src_ref=shifted.at[span], dst_ref=left.at[span],
            send_sem=x_send.at[0], recv_sem=x_recv.at[piece // X_GROUP],
            device_id=(i_next, j), device_id_type=MESH,
        )

    def x_copy(piece):
        span = pl.ds(piece * PIECE, PIECE)
        return pltpu.make_async_remote_copy(
            src_ref=shifted.at[span], dst_ref=left.at[span],
            send_sem=x_send.at[0], recv_sem=x_recv.at[piece // X_GROUP],
            device_id=(i_next, j), device_id_type=MESH,
        )

    def gather(source, start, target):
        picked = [
            source[part, bands[band], pl.ds(start, PREP), :]
            for part in range(2)
            for band in range(nband)
        ]
        block = jnp.stack(picked).astype(jnp.float32)
        plain[pl.ds(target, PREP)] = jnp.swapaxes(block, 0, 1).astype(jnp.bfloat16)

    at_once = jnp.where(lax.rem(i, 2) == 0, pieces - 1, 1)

    def send_plain(piece):
        @pl.when(piece < at_once)
        def _():
            z_copy(piece).start()

    def send_late(piece, _):
        z_copy(piece).start()
        return 0

    def z_last(part):
        span = pl.ds((pieces - 1) * PIECE + part * parts[0], parts[part])
        return pltpu.make_async_remote_copy(
            src_ref=plain.at[span], dst_ref=upper.at[span],
            send_sem=z_send.at[0], recv_sem=z_recv.at[part],
            device_id=(i, j_prev), device_id_type=MESH,
        )

    load_bands.wait()
    load_first.wait()
    gather(first, 0, 0)
    pl.semaphore_wait(barrier, len(partners))
    send_plain(0)
    load_rest.wait()
    load_umklapp.wait()

    def gather_step(step, _):
        gather(rest, pl.multiple_of((step - 1) * PREP, PREP), step * PREP)
        send_plain(step)
        return 0

    lax.fori_loop(1, rows // PREP, gather_step, 0)

    off_x = [jnp.where(i == nx - 1, umklapp[0, c], 0) for c in range(2)]
    off_y = [jnp.where(j == ny - 1, umklapp[1, c], 0) for c in range(2)]
    distance = lax.broadcasted_iota(jnp.int32, (cols, cols), 0) - lax.broadcasted_iota(
        jnp.int32, (cols, cols), 1
    )

    def mover(shift):
        far = distance - shift
        hit = (far == 0) | (far == cols) | (far == -cols)
        return jnp.where(hit, 1.0, 0.0).astype(jnp.bfloat16)

    def roll_group(target, start, shift, move):
        block = jnp.concatenate(
            [plain[lax.rem(start + k + shift + rows, rows)] for k in range(4)], axis=0
        )
        moved = jnp.dot(block, move, preferred_element_type=jnp.float32).astype(jnp.bfloat16)
        target[pl.ds(start, 4)] = moved.reshape(4, count, cols)

    move_far = mover(off_x[1] + off_y[1])

    def shift_step(piece, _):
        for k in range(PIECE // 4):
            roll_group(shifted, piece * PIECE + 4 * k, off_x[0] + off_y[0], move_far)
        x_copy(piece).start()
        return 0

    lax.fori_loop(0, pieces, shift_step, 0)
    move_near = mover(off_y[1])

    def local_step(step, _):
        roll_group(local, step * 4, off_y[0], move_near)
        return 0

    lax.fori_loop(0, rows // 8, local_step, 0)
    lax.fori_loop(at_once, pieces - 1, send_late, 0)
    z_last(0).start()
    z_last(1).start()
    lax.fori_loop(rows // 8, rows // 4, local_step, 0)

    def left_step(piece, total):
        @pl.when(lax.rem(piece, X_GROUP) == 0)
        def _():
            x_group(piece).wait_recv()

        for k in range(PIECE):
            row = piece * PIECE + k
            total = total + lax.dot_general(
                left[row], local[row], NT, preferred_element_type=jnp.float32
            )
        return total

    width = 2 * count
    back = width - nband

    def parted(square):
        wide = jnp.concatenate([square, square], axis=1)
        upper_half, lower_half = wide[:nband], wide[nband:]
        return (
            upper_half + pltpu.roll(lower_half, back, 1),
            pltpu.roll(upper_half, back, 1) - lower_half,
        )

    def mail_to(box, slot, index, device):
        return pltpu.make_async_remote_copy(
            src_ref=box, dst_ref=slot, send_sem=mail_send.at[index], recv_sem=mail_recv.at[index],
            device_id=device, device_id_type=MESH,
        )

    total_x = lax.fori_loop(0, pieces, left_step, jnp.zeros((count, count), jnp.float32))
    unit_re, unit_im = det_units(*parted(total_x))
    early[0:1] = unit_re
    early[1:2] = unit_im
    early_to_x = mail_to(early, early_x, 1, (i_prev, j))
    early_to_x.start()
    early_to_x.wait_recv()
    early_to_d = mail_to(early_x, early_d, 0, (i, j_prev))
    early_to_d.start()

    def add_row(row, total):
        sides = jnp.concatenate([left[row], local[row]], axis=0)
        return total + lax.dot_general(upper[row], sides, NT, preferred_element_type=jnp.float32)

    whole = (pieces - 1) // Z_GROUP * Z_GROUP

    def upper_step(piece, total):
        @pl.when((lax.rem(piece, Z_GROUP) == 0) & (piece < whole))
        def _():
            z_group(piece, Z_GROUP).wait_recv()

        @pl.when(piece == whole)
        def _():
            z_group(piece, pieces - 1 - whole).wait_recv()

        for k in range(PIECE):
            total = add_row(piece * PIECE + k, total)
        return total

    total = lax.fori_loop(0, pieces - 1, upper_step, jnp.zeros((count, width), jnp.float32))
    for part in range(2):
        z_last(part).wait_recv()
        for k in range(parts[part]):
            total = add_row((pieces - 1) * PIECE + part * parts[0] + k, total)
    over, under = total[:nband], total[nband:]
    unit_re, unit_im = det_units(
        over + pltpu.roll(under, back, 1), under - pltpu.roll(over, back, 1)
    )
    late[0:1] = unit_re
    late[1:2] = unit_im
    late_to_x = mail_to(late, late_x, 2, (i_prev, j))
    late_to_x.start()

    pltpu.make_async_remote_copy(
        src_ref=plain, dst_ref=upper, send_sem=z_send.at[0], recv_sem=z_recv.at[0],
        device_id=(i, j_prev), device_id_type=MESH,
    ).wait_send()
    pltpu.make_async_remote_copy(
        src_ref=shifted, dst_ref=left, send_sem=x_send.at[0], recv_sem=x_recv.at[0],
        device_id=(i_next, j), device_id_type=MESH,
    ).wait_send()
    early_to_x.wait_send()
    early_to_d.wait()
    along_y = (pltpu.roll(unit_re, count, 1), pltpu.roll(unit_im, count, 1))
    along_x = (early_x[0:1], early_x[1:2])
    x_next = (early_d[0:1], early_d[1:2])
    rest_of_second = times(conjugate(x_next), conjugate(along_y))
    late_to_x.wait_recv()
    late_re, late_im = late_x[0:1], late_x[1:2]
    along_d = (late_re, late_im)
    y_next = (pltpu.roll(late_re, count, 1), pltpu.roll(late_im, count, 1))
    one = times(times(along_x, y_next), conjugate(along_d))
    two = times(along_d, rest_of_second)
    at_zero = lax.broadcasted_iota(jnp.int32, (1, width), 1) == 0
    angle = jnp.arctan2(jnp.where(at_zero, one[1], two[1]), jnp.where(at_zero, one[0], two[0]))
    spot = lax.broadcasted_iota(jnp.int32, (1, width), 1)

    def placed(part):
        return jnp.where(
            spot == 0, along_x[part], jnp.where(spot == 1, along_y[part], along_d[part])
        )

    out[0:1] = angle
    out[1:2] = placed(0)
    out[2:3] = placed(1)
    out[3:8] = jnp.zeros((5, width), jnp.float32)
    late_to_x.wait_send()


def split(found, flux, links):
    flux[0] = found[0:1, :2]
    links[0, 0] = found[1:3, :3]


def det_units(work_re, work_im):
    nband, width = work_re.shape
    tiles = nband // 8
    re = [work_re[8 * g : 8 * g + 8] for g in range(tiles)]
    im = [work_im[8 * g : 8 * g + 8] for g in range(tiles)]
    lane8 = lax.broadcasted_iota(jnp.int32, (8, width), 1)
    group_start = lane8 - lax.rem(lane8, nband)
    unit = (jnp.ones((1, width), jnp.float32), jnp.zeros((1, width), jnp.float32))
    for g0 in range(tiles):
        live = range(g0, tiles)
        cols = []
        for m in range(8):
            place = group_start + (8 * g0 + m)
            cols.append({
                g: (
                    jnp.take_along_axis(re[g], place, axis=1),
                    jnp.take_along_axis(im[g], place, axis=1),
                )
                for g in live
            })
        for m in range(8):
            pr, pi = cols[m][g0][0][m : m + 1], cols[m][g0][1][m : m + 1]
            square = pr * pr + pi * pi
            scale = lax.rsqrt(square)
            unit = times(unit, (pr * scale, pi * scale))
            if 8 * g0 + m == nband - 1:
                break
            inverse = 1.0 / square
            against = {g: times(cols[m][g], (pr, -pi)) for g in live}
            factor = {g: (against[g][0] * inverse, against[g][1] * inverse) for g in live}
            for n in range(m + 1, 8):
                row = (cols[n][g0][0][m : m + 1], cols[n][g0][1][m : m + 1])
                for g in live:
                    if n == m + 1 and g == g0:
                        less = times(against[g], row)
                        less = (less[0] * inverse, less[1] * inverse)
                    else:
                        less = times(factor[g], row)
                    cols[n][g] = (cols[n][g][0] - less[0], cols[n][g][1] - less[1])
            if g0 + 1 < tiles:
                row = (re[g0][m : m + 1], im[g0][m : m + 1])
                for g in live:
                    less = times(factor[g], row)
                    re[g] = re[g] - less[0]
                    im[g] = im[g] - less[1]
    size = 1.0 / jnp.sqrt(unit[0] * unit[0] + unit[1] * unit[1])
    return unit[0] * size, unit[1] * size


def times(first, second):
    return (
        first[0] * second[0] - first[1] * second[1],
        first[0] * second[1] + first[1] * second[0],
    )


def conjugate(value):
    return (value[0], -value[1])


def per_device(coeffs, bands, umklapp):
    block = coeffs[0, 0]
    rows, cols = block.shape[2], block.shape[3]
    nstore, nband = block.shape[1], bands.shape[0]
    count = 2 * nband
    pieces = rows // PIECE
    side = pltpu.VMEM((rows, count, cols), jnp.bfloat16)
    tile = pltpu.VMEM((8, 2 * count), jnp.float32)
    found = pl.pallas_call(
        kernel,
        out_shape=pltpu.VMEM((8, 2 * count), jnp.float32),
        in_specs=[pl.BlockSpec(memory_space=pl.ANY)] * 3,
        out_specs=pl.BlockSpec(memory_space=pltpu.VMEM),
        scratch_shapes=[
            pltpu.SMEM(bands.shape, jnp.int32),
            pltpu.SMEM(umklapp.shape, jnp.int32),
            pltpu.VMEM((2, nstore, PREP, cols), jnp.bfloat16),
            pltpu.VMEM((2, nstore, rows - PREP, cols), jnp.bfloat16),
            side, side, side, side, side,
            tile, tile, tile, tile, tile,
            pltpu.SemaphoreType.DMA((4,)),
            pltpu.SemaphoreType.DMA((1,)),
            pltpu.SemaphoreType.DMA((2 + pieces // Z_GROUP,)),
            pltpu.SemaphoreType.DMA((1,)),
            pltpu.SemaphoreType.DMA((pieces // X_GROUP,)),
            pltpu.SemaphoreType.DMA((3,)),
            pltpu.SemaphoreType.DMA((3,)),
        ],
        compiler_params=pltpu.CompilerParams(
            collective_id=0, has_side_effects=True, vmem_limit_bytes=56 * 1024 * 1024
        ),
    )(block, bands, umklapp)
    flux, links = pl.pallas_call(
        split,
        out_shape=(
            jax.ShapeDtypeStruct((1, 1, 2), jnp.float32),
            jax.ShapeDtypeStruct((1, 1, 2, 3), jnp.float32),
        ),
        in_specs=[pl.BlockSpec(memory_space=pltpu.VMEM)],
        out_specs=(
            pl.BlockSpec(memory_space=pltpu.VMEM),
            pl.BlockSpec(memory_space=pltpu.VMEM),
        ),
        compiler_params=pltpu.CompilerParams(vmem_limit_bytes=1024 * 1024),
    )(found)
    return (flux, jnp.swapaxes(links, 2, 3))


def solution(mesh):
    in_specs = (P("kx", "ky", None, None, None, None), P(), P())
    out_specs = (P("kx", "ky", None), P("kx", "ky", None, None))
    return jax.shard_map(
        per_device, mesh=mesh, in_specs=in_specs, out_specs=out_specs, check_vma=False
    )
```

```python
import functools

import jax
import jax.numpy as jnp
from jax import lax
from jax.experimental import pallas as pl
from jax.experimental.pallas import tpu as pltpu
from jax.sharding import PartitionSpec as P

MESH = pl.DeviceIdType.MESH
NT = (((1,), (1,)), ((), ()))
PREP = 8
PIECE = 8
LAST = 2
X_GROUP = 4
Z_GROUP = 2


def kernel(
    coeffs, bands_far, umklapp_far, out,
    bands, umklapp, first, rest, plain, local, shifted, upper, left, early, late, early_x, early_d, late_x,
    load_sem, z_send, z_recv, x_send, x_recv, mail_send, mail_recv,
):
    rows, count, cols = plain.shape
    nband = bands.shape[0]
    pieces = rows // PIECE
    parts = (PIECE - LAST, LAST)
    nx, ny = lax.axis_size("kx"), lax.axis_size("ky")
    i, j = lax.axis_index("kx"), lax.axis_index("ky")
    i_next, i_prev = lax.rem(i + 1, nx), lax.rem(i + nx - 1, nx)
    j_next, j_prev = lax.rem(j + 1, ny), lax.rem(j + ny - 1, ny)

    load_first = pltpu.make_async_copy(
        coeffs.at[:, :, pl.ds(0, PREP)], first, load_sem.at[0]
    )
    load_rest = pltpu.make_async_copy(
        coeffs.at[:, :, pl.ds(PREP, rows - PREP)], rest, load_sem.at[1]
    )
    load_bands = pltpu.make_async_copy(bands_far, bands, load_sem.at[2])
    load_umklapp = pltpu.make_async_copy(umklapp_far, umklapp, load_sem.at[3])
    barrier = pltpu.get_barrier_semaphore()
    partners = [(i, j_next), (i_prev, j)]
    for partner in partners:
        pl.semaphore_signal(barrier, inc=1, device_id=partner, device_id_type=MESH)

    load_bands.start()
    load_first.start()
    load_umklapp.start()
    load_rest.start()

    def z_copy(piece):
        span = pl.ds(piece * PIECE, PIECE)
        return pltpu.make_async_remote_copy(
            src_ref=plain.at[span], dst_ref=upper.at[span],
            send_sem=z_send.at[0], recv_sem=z_recv.at[2 + piece // Z_GROUP],
            device_id=(i, j_prev), device_id_type=MESH,
        )

    def z_group(piece, size):
        span = pl.ds(piece * PIECE, size * PIECE)
        return pltpu.make_async_remote_copy(
            src_ref=plain.at[span], dst_ref=upper.at[span],
            send_sem=z_send.at[0], recv_sem=z_recv.at[2 + piece // Z_GROUP],
            device_id=(i, j_prev), device_id_type=MESH,
        )

    def x_group(piece):
        span = pl.ds(piece * PIECE, X_GROUP * PIECE)
        return pltpu.make_async_remote_copy(
            src_ref=shifted.at[span], dst_ref=left.at[span],
            send_sem=x_send.at[0], recv_sem=x_recv.at[piece // X_GROUP],
            device_id=(i_next, j), device_id_type=MESH,
        )

    def x_copy(piece):
        span = pl.ds(piece * PIECE, PIECE)
        return pltpu.make_async_remote_copy(
            src_ref=shifted.at[span], dst_ref=left.at[span],
            send_sem=x_send.at[0], recv_sem=x_recv.at[piece // X_GROUP],
            device_id=(i_next, j), device_id_type=MESH,
        )

    def gather(source, start, target):
        picked = [
            source[part, bands[band], pl.ds(start, PREP), :]
            for part in range(2)
            for band in range(nband)
        ]
        block = jnp.stack(picked).astype(jnp.float32)
        plain[pl.ds(target, PREP)] = jnp.swapaxes(block, 0, 1).astype(jnp.bfloat16)

    at_once = jnp.where(lax.rem(i, 2) == 0, pieces - 1, 1)

    def send_plain(piece):
        @pl.when(piece < at_once)
        def _():
            z_copy(piece).start()

    def send_late(piece, _):
        z_copy(piece).start()
        return 0

    def z_last(part):
        span = pl.ds((pieces - 1) * PIECE + part * parts[0], parts[part])
        return pltpu.make_async_remote_copy(
            src_ref=plain.at[span], dst_ref=upper.at[span],
            send_sem=z_send.at[0], recv_sem=z_recv.at[part],
            device_id=(i, j_prev), device_id_type=MESH,
        )

    load_bands.wait()
    load_first.wait()
    gather(first, 0, 0)
    pl.semaphore_wait(barrier, len(partners))
    send_plain(0)
    load_rest.wait()
    load_umklapp.wait()

    def gather_step(step, _):
        gather(rest, pl.multiple_of((step - 1) * PREP, PREP), step * PREP)
        send_plain(step)
        return 0

    lax.fori_loop(1, rows // PREP, gather_step, 0)

    off_x = [jnp.where(i == nx - 1, umklapp[0, c], 0) for c in range(2)]
    off_y = [jnp.where(j == ny - 1, umklapp[1, c], 0) for c in range(2)]
    distance = lax.broadcasted_iota(jnp.int32, (cols, cols), 0) - lax.broadcasted_iota(
        jnp.int32, (cols, cols), 1
    )

    def mover(shift):
        far = distance - shift
        hit = (far == 0) | (far == cols) | (far == -cols)
        return jnp.where(hit, 1.0, 0.0).astype(jnp.bfloat16)

    def roll_group(target, start, shift, move):
        block = jnp.concatenate(
            [plain[lax.rem(start + k + shift + rows, rows)] for k in range(4)], axis=0
        )
        moved = jnp.dot(block, move, preferred_element_type=jnp.float32).astype(jnp.bfloat16)
        target[pl.ds(start, 4)] = moved.reshape(4, count, cols)

    move_far = mover(off_x[1] + off_y[1])

    def shift_step(piece, _):
        for k in range(PIECE // 4):
            roll_group(shifted, piece * PIECE + 4 * k, off_x[0] + off_y[0], move_far)
        x_copy(piece).start()
        return 0

    lax.fori_loop(0, pieces, shift_step, 0)
    move_near = mover(off_y[1])

    def local_step(step, _):
        roll_group(local, step * 4, off_y[0], move_near)
        return 0

    lax.fori_loop(0, rows // 8, local_step, 0)
    lax.fori_loop(at_once, pieces - 1, send_late, 0)
    z_last(0).start()
    z_last(1).start()
    lax.fori_loop(rows // 8, rows // 4, local_step, 0)

    def left_step(piece, total):
        @pl.when(lax.rem(piece, X_GROUP) == 0)
        def _():
            x_group(piece).wait_recv()

        for k in range(PIECE):
            row = piece * PIECE + k
            total = total + lax.dot_general(
                left[row], local[row], NT, preferred_element_type=jnp.float32
            )
        return total

    width = 2 * count
    back = width - nband

    def parted(square):
        wide = jnp.concatenate([square, square], axis=1)
        upper_half, lower_half = wide[:nband], wide[nband:]
        return (
            upper_half + pltpu.roll(lower_half, back, 1),
            pltpu.roll(upper_half, back, 1) - lower_half,
        )

    def mail_to(box, slot, index, device):
        return pltpu.make_async_remote_copy(
            src_ref=box, dst_ref=slot, send_sem=mail_send.at[index], recv_sem=mail_recv.at[index],
            device_id=device, device_id_type=MESH,
        )

    total_x = lax.fori_loop(0, pieces, left_step, jnp.zeros((count, count), jnp.float32))
    unit_re, unit_im = det_units(*parted(total_x))
    early[0:1] = unit_re
    early[1:2] = unit_im
    early_to_x = mail_to(early, early_x, 1, (i_prev, j))
    early_to_x.start()
    early_to_x.wait_recv()
    early_to_d = mail_to(early_x, early_d, 0, (i, j_prev))
    early_to_d.start()

    def add_row(row, total):
        sides = jnp.concatenate([left[row], local[row]], axis=0)
        return total + lax.dot_general(upper[row], sides, NT, preferred_element_type=jnp.float32)

    whole = (pieces - 1) // Z_GROUP * Z_GROUP

    def upper_step(piece, total):
        @pl.when((lax.rem(piece, Z_GROUP) == 0) & (piece < whole))
        def _():
            z_group(piece, Z_GROUP).wait_recv()

        @pl.when(piece == whole)
        def _():
            z_group(piece, pieces - 1 - whole).wait_recv()

        for k in range(PIECE):
            total = add_row(piece * PIECE + k, total)
        return total

    total = lax.fori_loop(0, pieces - 1, upper_step, jnp.zeros((count, width), jnp.float32))
    for part in range(2):
        z_last(part).wait_recv()
        for k in range(parts[part]):
            total = add_row((pieces - 1) * PIECE + part * parts[0] + k, total)
    over, under = total[:nband], total[nband:]
    unit_re, unit_im = det_units(
        over + pltpu.roll(under, back, 1), under - pltpu.roll(over, back, 1)
    )
    late[0:1] = unit_re
    late[1:2] = unit_im
    late_to_x = mail_to(late, late_x, 2, (i_prev, j))
    late_to_x.start()

    pltpu.make_async_remote_copy(
        src_ref=plain, dst_ref=upper, send_sem=z_send.at[0], recv_sem=z_recv.at[0],
        device_id=(i, j_prev), device_id_type=MESH,
    ).wait_send()
    pltpu.make_async_remote_copy(
        src_ref=shifted, dst_ref=left, send_sem=x_send.at[0], recv_sem=x_recv.at[0],
        device_id=(i_next, j), device_id_type=MESH,
    ).wait_send()
    early_to_x.wait_send()
    early_to_d.wait()
    along_y = (pltpu.roll(unit_re, count, 1), pltpu.roll(unit_im, count, 1))
    along_x = (early_x[0:1], early_x[1:2])
    x_next = (early_d[0:1], early_d[1:2])
    rest_of_second = times(conjugate(x_next), conjugate(along_y))
    late_to_x.wait_recv()
    late_re, late_im = late_x[0:1], late_x[1:2]
    along_d = (late_re, late_im)
    y_next = (pltpu.roll(late_re, count, 1), pltpu.roll(late_im, count, 1))
    one = times(times(along_x, y_next), conjugate(along_d))
    two = times(along_d, rest_of_second)
    at_zero = lax.broadcasted_iota(jnp.int32, (1, width), 1) == 0
    angle = jnp.arctan2(jnp.where(at_zero, one[1], two[1]), jnp.where(at_zero, one[0], two[0]))
    spot = lax.broadcasted_iota(jnp.int32, (1, width), 1)

    def placed(part):
        return jnp.where(
            spot == 0, along_x[part], jnp.where(spot == 1, along_y[part], along_d[part])
        )

    out[0:1] = angle
    out[1:2] = placed(0)
    out[2:3] = placed(1)
    out[3:8] = jnp.zeros((5, width), jnp.float32)
    late_to_x.wait_send()


def split(found, flux, links):
    flux[0] = found[0:1, :2]
    links[0, 0] = found[1:3, :3]


def det_units(work_re, work_im):
    nband, width = work_re.shape
    tiles = nband // 8
    re = [work_re[8 * g : 8 * g + 8] for g in range(tiles)]
    im = [work_im[8 * g : 8 * g + 8] for g in range(tiles)]
    lane8 = lax.broadcasted_iota(jnp.int32, (8, width), 1)
    group_start = lane8 - lax.rem(lane8, nband)
    unit = (jnp.ones((1, width), jnp.float32), jnp.zeros((1, width), jnp.float32))
    for g0 in range(tiles):
        live = range(g0, tiles)
        if g0 == tiles - 1:
            size = 1.0 / jnp.sqrt(unit[0] * unit[0] + unit[1] * unit[1])
            unit = (unit[0] * size, unit[1] * size)
        cols = []
        for m in range(8):
            place = group_start + (8 * g0 + m)
            cols.append({
                g: (
                    jnp.take_along_axis(re[g], place, axis=1),
                    jnp.take_along_axis(im[g], place, axis=1),
                )
                for g in live
            })
        for m in range(8):
            pr, pi = cols[m][g0][0][m : m + 1], cols[m][g0][1][m : m + 1]
            square = pr * pr + pi * pi
            scale = lax.rsqrt(square)
            unit = times(unit, (pr * scale, pi * scale))
            if 8 * g0 + m == nband - 1:
                break
            inverse = 1.0 / square
            against = {g: times(cols[m][g], (pr, -pi)) for g in live}
            factor = {g: (against[g][0] * inverse, against[g][1] * inverse) for g in live}
            for n in range(m + 1, 8):
                row = (cols[n][g0][0][m : m + 1], cols[n][g0][1][m : m + 1])
                for g in live:
                    if n == m + 1 and g == g0:
                        less = times(against[g], row)
                        less = (less[0] * inverse, less[1] * inverse)
                    else:
                        less = times(factor[g], row)
                    cols[n][g] = (cols[n][g][0] - less[0], cols[n][g][1] - less[1])
            if g0 + 1 < tiles:
                row = (re[g0][m : m + 1], im[g0][m : m + 1])
                for g in live:
                    less = times(factor[g], row)
                    re[g] = re[g] - less[0]
                    im[g] = im[g] - less[1]
    return unit


def times(first, second):
    return (
        first[0] * second[0] - first[1] * second[1],
        first[0] * second[1] + first[1] * second[0],
    )


def conjugate(value):
    return (value[0], -value[1])


def per_device(coeffs, bands, umklapp):
    block = coeffs[0, 0]
    rows, cols = block.shape[2], block.shape[3]
    nstore, nband = block.shape[1], bands.shape[0]
    count = 2 * nband
    pieces = rows // PIECE
    side = pltpu.VMEM((rows, count, cols), jnp.bfloat16)
    tile = pltpu.VMEM((8, 2 * count), jnp.float32)
    found = pl.pallas_call(
        kernel,
        out_shape=pltpu.VMEM((8, 2 * count), jnp.float32),
        in_specs=[pl.BlockSpec(memory_space=pl.ANY)] * 3,
        out_specs=pl.BlockSpec(memory_space=pltpu.VMEM),
        scratch_shapes=[
            pltpu.SMEM(bands.shape, jnp.int32),
            pltpu.SMEM(umklapp.shape, jnp.int32),
            pltpu.VMEM((2, nstore, PREP, cols), jnp.bfloat16),
            pltpu.VMEM((2, nstore, rows - PREP, cols), jnp.bfloat16),
            side, side, side, side, side,
            tile, tile, tile, tile, tile,
            pltpu.SemaphoreType.DMA((4,)),
            pltpu.SemaphoreType.DMA((1,)),
            pltpu.SemaphoreType.DMA((2 + pieces // Z_GROUP,)),
            pltpu.SemaphoreType.DMA((1,)),
            pltpu.SemaphoreType.DMA((pieces // X_GROUP,)),
            pltpu.SemaphoreType.DMA((3,)),
            pltpu.SemaphoreType.DMA((3,)),
        ],
        compiler_params=pltpu.CompilerParams(
            collective_id=0, has_side_effects=True, vmem_limit_bytes=56 * 1024 * 1024
        ),
    )(block, bands, umklapp)
    flux, links = pl.pallas_call(
        split,
        out_shape=(
            jax.ShapeDtypeStruct((1, 1, 2), jnp.float32),
            jax.ShapeDtypeStruct((1, 1, 2, 3), jnp.float32),
        ),
        in_specs=[pl.BlockSpec(memory_space=pltpu.VMEM)],
        out_specs=(
            pl.BlockSpec(memory_space=pltpu.VMEM),
            pl.BlockSpec(memory_space=pltpu.VMEM),
        ),
        compiler_params=pltpu.CompilerParams(vmem_limit_bytes=1024 * 1024),
    )(found)
    return (flux, jnp.swapaxes(links, 2, 3))


def solution(mesh):
    in_specs = (P("kx", "ky", None, None, None, None), P(), P())
    out_specs = (P("kx", "ky", None), P("kx", "ky", None, None))
    return jax.shard_map(
        per_device, mesh=mesh, in_specs=in_specs, out_specs=out_specs, check_vma=False
    )
```

```python
import functools

import jax
import jax.numpy as jnp
from jax import lax
from jax.experimental import pallas as pl
from jax.experimental.pallas import tpu as pltpu
from jax.sharding import PartitionSpec as P

MESH = pl.DeviceIdType.MESH
NT = (((1,), (1,)), ((), ()))
PREP = 8
PIECE = 8
LAST = 2
X_GROUP = 4
Z_GROUP = 2


def kernel(
    coeffs, bands_far, umklapp_far, out,
    bands, umklapp, first, rest, plain, local, shifted, upper, left, early, late, early_x, early_d, late_x,
    load_sem, z_send, z_recv, x_send, x_recv, mail_send, mail_recv,
):
    rows, count, cols = plain.shape
    nband = bands.shape[0]
    pieces = rows // PIECE
    parts = (PIECE - LAST, LAST)
    nx, ny = lax.axis_size("kx"), lax.axis_size("ky")
    i, j = lax.axis_index("kx"), lax.axis_index("ky")
    i_next, i_prev = lax.rem(i + 1, nx), lax.rem(i + nx - 1, nx)
    j_next, j_prev = lax.rem(j + 1, ny), lax.rem(j + ny - 1, ny)

    load_first = pltpu.make_async_copy(
        coeffs.at[:, :, pl.ds(0, PREP)], first, load_sem.at[0]
    )
    load_rest = pltpu.make_async_copy(
        coeffs.at[:, :, pl.ds(PREP, rows - PREP)], rest, load_sem.at[1]
    )
    load_bands = pltpu.make_async_copy(bands_far, bands, load_sem.at[2])
    load_umklapp = pltpu.make_async_copy(umklapp_far, umklapp, load_sem.at[3])
    barrier = pltpu.get_barrier_semaphore()
    partners = [(i, j_next), (i_prev, j)]
    for partner in partners:
        pl.semaphore_signal(barrier, inc=1, device_id=partner, device_id_type=MESH)

    load_bands.start()
    load_first.start()
    load_umklapp.start()
    load_rest.start()

    def z_copy(piece):
        span = pl.ds(piece * PIECE, PIECE)
        return pltpu.make_async_remote_copy(
            src_ref=plain.at[span], dst_ref=upper.at[span],
            send_sem=z_send.at[0], recv_sem=z_recv.at[2 + piece // Z_GROUP],
            device_id=(i, j_prev), device_id_type=MESH,
        )

    def z_group(piece, size):
        span = pl.ds(piece * PIECE, size * PIECE)
        return pltpu.make_async_remote_copy(
            src_ref=plain.at[span], dst_ref=upper.at[span],
            send_sem=z_send.at[0], recv_sem=z_recv.at[2 + piece // Z_GROUP],
            device_id=(i, j_prev), device_id_type=MESH,
        )

    def x_group(piece):
        span = pl.ds(piece * PIECE, X_GROUP * PIECE)
        return pltpu.make_async_remote_copy(
            src_ref=shifted.at[span], dst_ref=left.at[span],
            send_sem=x_send.at[0], recv_sem=x_recv.at[piece // X_GROUP],
            device_id=(i_next, j), device_id_type=MESH,
        )

    def x_copy(piece):
        span = pl.ds(piece * PIECE, PIECE)
        return pltpu.make_async_remote_copy(
            src_ref=shifted.at[span], dst_ref=left.at[span],
            send_sem=x_send.at[0], recv_sem=x_recv.at[piece // X_GROUP],
            device_id=(i_next, j), device_id_type=MESH,
        )

    def gather(source, start, target):
        picked = [
            source[part, bands[band], pl.ds(start, PREP), :]
            for part in range(2)
            for band in range(nband)
        ]
        block = jnp.stack(picked).astype(jnp.float32)
        plain[pl.ds(target, PREP)] = jnp.swapaxes(block, 0, 1).astype(jnp.bfloat16)

    at_once = jnp.where(lax.rem(i, 2) == 0, pieces - 1, 1)

    def send_plain(piece):
        @pl.when(piece < at_once)
        def _():
            z_copy(piece).start()

    def send_late(piece, _):
        z_copy(piece).start()
        return 0

    def z_last(part):
        span = pl.ds((pieces - 1) * PIECE + part * parts[0], parts[part])
        return pltpu.make_async_remote_copy(
            src_ref=plain.at[span], dst_ref=upper.at[span],
            send_sem=z_send.at[0], recv_sem=z_recv.at[part],
            device_id=(i, j_prev), device_id_type=MESH,
        )

    load_bands.wait()
    load_first.wait()
    gather(first, 0, 0)
    pl.semaphore_wait(barrier, len(partners))
    send_plain(0)
    load_rest.wait()
    load_umklapp.wait()

    def gather_step(step, _):
        gather(rest, pl.multiple_of((step - 1) * PREP, PREP), step * PREP)
        send_plain(step)
        return 0

    lax.fori_loop(1, rows // PREP, gather_step, 0)

    off_x = [jnp.where(i == nx - 1, umklapp[0, c], 0) for c in range(2)]
    off_y = [jnp.where(j == ny - 1, umklapp[1, c], 0) for c in range(2)]
    distance = lax.broadcasted_iota(jnp.int32, (cols, cols), 0) - lax.broadcasted_iota(
        jnp.int32, (cols, cols), 1
    )

    def mover(shift):
        far = distance - shift
        hit = (far == 0) | (far == cols) | (far == -cols)
        return jnp.where(hit, 1.0, 0.0).astype(jnp.bfloat16)

    def roll_group(target, start, shift, move):
        block = jnp.concatenate(
            [plain[lax.rem(start + k + shift + rows, rows)] for k in range(4)], axis=0
        )
        moved = jnp.dot(block, move, preferred_element_type=jnp.float32).astype(jnp.bfloat16)
        target[pl.ds(start, 4)] = moved.reshape(4, count, cols)

    move_far = mover(off_x[1] + off_y[1])

    def shift_step(piece, _):
        for k in range(PIECE // 4):
            roll_group(shifted, piece * PIECE + 4 * k, off_x[0] + off_y[0], move_far)
        x_copy(piece).start()
        return 0

    lax.fori_loop(0, pieces, shift_step, 0)
    move_near = mover(off_y[1])

    def local_step(step, _):
        roll_group(local, step * 4, off_y[0], move_near)
        return 0

    lax.fori_loop(0, rows // 8, local_step, 0)
    lax.fori_loop(at_once, pieces - 1, send_late, 0)
    z_last(0).start()
    z_last(1).start()
    lax.fori_loop(rows // 8, rows // 4, local_step, 0)

    def left_step(piece, total):
        @pl.when(lax.rem(piece, X_GROUP) == 0)
        def _():
            x_group(piece).wait_recv()

        for k in range(PIECE):
            row = piece * PIECE + k
            total = total + lax.dot_general(
                left[row], local[row], NT, preferred_element_type=jnp.float32
            )
        return total

    width = 2 * count
    back = width - nband

    def parted(square):
        wide = jnp.concatenate([square, square], axis=1)
        upper_half, lower_half = wide[:nband], wide[nband:]
        return (
            upper_half + pltpu.roll(lower_half, back, 1),
            pltpu.roll(upper_half, back, 1) - lower_half,
        )

    def mail_to(box, slot, index, device):
        return pltpu.make_async_remote_copy(
            src_ref=box, dst_ref=slot, send_sem=mail_send.at[index], recv_sem=mail_recv.at[index],
            device_id=device, device_id_type=MESH,
        )

    total_x = lax.fori_loop(0, pieces, left_step, jnp.zeros((count, count), jnp.float32))
    unit_re, unit_im = det_units(*parted(total_x))
    early[0:1] = unit_re
    early[1:2] = unit_im
    early_to_x = mail_to(early, early_x, 1, (i_prev, j))
    early_to_x.start()
    early_to_x.wait_recv()
    early_to_d = mail_to(early_x, early_d, 0, (i, j_prev))
    early_to_d.start()

    def add_row(row, total):
        sides = jnp.concatenate([left[row], local[row]], axis=0)
        return total + lax.dot_general(upper[row], sides, NT, preferred_element_type=jnp.float32)

    whole = (pieces - 1) // Z_GROUP * Z_GROUP

    def upper_step(piece, total):
        @pl.when((lax.rem(piece, Z_GROUP) == 0) & (piece < whole))
        def _():
            z_group(piece, Z_GROUP).wait_recv()

        @pl.when(piece == whole)
        def _():
            z_group(piece, pieces - 1 - whole).wait_recv()

        for k in range(PIECE):
            total = add_row(piece * PIECE + k, total)
        return total

    total = lax.fori_loop(0, pieces - 1, upper_step, jnp.zeros((count, width), jnp.float32))
    for part in range(2):
        z_last(part).wait_recv()
        for k in range(parts[part]):
            total = add_row((pieces - 1) * PIECE + part * parts[0] + k, total)
    over, under = total[:nband], total[nband:]
    unit_d, along_y = det_units(
        over + pltpu.roll(under, back, 1), under - pltpu.roll(over, back, 1), (0, count)
    )
    for part in range(2):
        late[part : part + 1] = unit_d[part]
        late[2 + part : 3 + part] = along_y[part]
    late_to_x = mail_to(late, late_x, 2, (i_prev, j))
    late_to_x.start()

    pltpu.make_async_remote_copy(
        src_ref=plain, dst_ref=upper, send_sem=z_send.at[0], recv_sem=z_recv.at[0],
        device_id=(i, j_prev), device_id_type=MESH,
    ).wait_send()
    pltpu.make_async_remote_copy(
        src_ref=shifted, dst_ref=left, send_sem=x_send.at[0], recv_sem=x_recv.at[0],
        device_id=(i_next, j), device_id_type=MESH,
    ).wait_send()
    early_to_x.wait_send()
    early_to_d.wait()
    along_x = (early_x[0:1], early_x[1:2])
    x_next = (early_d[0:1], early_d[1:2])
    rest_of_second = times(conjugate(x_next), conjugate(along_y))
    late_to_x.wait_recv()
    along_d = (late_x[0:1], late_x[1:2])
    y_next = (late_x[2:3], late_x[3:4])
    one = times(times(along_x, y_next), conjugate(along_d))
    two = times(along_d, rest_of_second)
    at_zero = lax.broadcasted_iota(jnp.int32, (1, width), 1) == 0
    angle = jnp.arctan2(jnp.where(at_zero, one[1], two[1]), jnp.where(at_zero, one[0], two[0]))
    spot = lax.broadcasted_iota(jnp.int32, (1, width), 1)

    def placed(part):
        return jnp.where(
            spot == 0, along_x[part], jnp.where(spot == 1, along_y[part], along_d[part])
        )

    out[0:1] = angle
    out[1:2] = placed(0)
    out[2:3] = placed(1)
    out[3:8] = jnp.zeros((5, width), jnp.float32)
    late_to_x.wait_send()


def split(found, flux, links):
    flux[0] = found[0:1, :2]
    links[0, 0] = found[1:3, :3]


def det_units(work_re, work_im, starts=None):
    nband, width = work_re.shape
    tiles = nband // 8
    re = [work_re[8 * g : 8 * g + 8] for g in range(tiles)]
    im = [work_im[8 * g : 8 * g + 8] for g in range(tiles)]
    lane8 = lax.broadcasted_iota(jnp.int32, (8, width), 1)
    group_start = lane8 - lax.rem(lane8, nband)
    unit = (jnp.ones((1, width), jnp.float32), jnp.zeros((1, width), jnp.float32))
    for g0 in range(tiles):
        live = range(g0, tiles)
        if g0 == tiles - 1:
            size = 1.0 / jnp.sqrt(unit[0] * unit[0] + unit[1] * unit[1])
            unit = (unit[0] * size, unit[1] * size)
            if starts is not None:
                return [last_panel(re[g0], im[g0], unit, lane8 * 0 + start, nband) for start in starts]
        cols = []
        for m in range(8):
            place = group_start + (8 * g0 + m)
            cols.append({
                g: (
                    jnp.take_along_axis(re[g], place, axis=1),
                    jnp.take_along_axis(im[g], place, axis=1),
                )
                for g in live
            })
        for m in range(8):
            pr, pi = cols[m][g0][0][m : m + 1], cols[m][g0][1][m : m + 1]
            square = pr * pr + pi * pi
            scale = lax.rsqrt(square)
            unit = times(unit, (pr * scale, pi * scale))
            if 8 * g0 + m == nband - 1:
                break
            inverse = 1.0 / square
            against = {g: times(cols[m][g], (pr, -pi)) for g in live}
            factor = {g: (against[g][0] * inverse, against[g][1] * inverse) for g in live}
            for n in range(m + 1, 8):
                row = (cols[n][g0][0][m : m + 1], cols[n][g0][1][m : m + 1])
                for g in live:
                    if n == m + 1 and g == g0:
                        less = times(against[g], row)
                        less = (less[0] * inverse, less[1] * inverse)
                    else:
                        less = times(factor[g], row)
                    cols[n][g] = (cols[n][g][0] - less[0], cols[n][g][1] - less[1])
            if g0 + 1 < tiles:
                row = (re[g0][m : m + 1], im[g0][m : m + 1])
                for g in live:
                    less = times(factor[g], row)
                    re[g] = re[g] - less[0]
                    im[g] = im[g] - less[1]
    return unit


def last_panel(re, im, unit, start, nband):
    def spread(value, place):
        return jnp.take_along_axis(value, place, axis=1)

    cols = [(spread(re, start + nband - 8 + m), spread(im, start + nband - 8 + m)) for m in range(8)]
    unit = tuple(spread(jnp.broadcast_to(part, re.shape), start)[0:1] for part in unit)
    for m in range(8):
        pr, pi = cols[m][0][m : m + 1], cols[m][1][m : m + 1]
        square = pr * pr + pi * pi
        scale = lax.rsqrt(square)
        unit = times(unit, (pr * scale, pi * scale))
        if m == 7:
            return unit
        inverse = 1.0 / square
        against = times(cols[m], (pr, -pi))
        factor = (against[0] * inverse, against[1] * inverse)
        for n in range(m + 1, 8):
            row = (cols[n][0][m : m + 1], cols[n][1][m : m + 1])
            if n == m + 1:
                less = times(against, row)
                less = (less[0] * inverse, less[1] * inverse)
            else:
                less = times(factor, row)
            cols[n] = (cols[n][0] - less[0], cols[n][1] - less[1])


def times(first, second):
    return (
        first[0] * second[0] - first[1] * second[1],
        first[0] * second[1] + first[1] * second[0],
    )


def conjugate(value):
    return (value[0], -value[1])


def per_device(coeffs, bands, umklapp):
    block = coeffs[0, 0]
    rows, cols = block.shape[2], block.shape[3]
    nstore, nband = block.shape[1], bands.shape[0]
    count = 2 * nband
    pieces = rows // PIECE
    side = pltpu.VMEM((rows, count, cols), jnp.bfloat16)
    tile = pltpu.VMEM((8, 2 * count), jnp.float32)
    found = pl.pallas_call(
        kernel,
        out_shape=pltpu.VMEM((8, 2 * count), jnp.float32),
        in_specs=[pl.BlockSpec(memory_space=pl.ANY)] * 3,
        out_specs=pl.BlockSpec(memory_space=pltpu.VMEM),
        scratch_shapes=[
            pltpu.SMEM(bands.shape, jnp.int32),
            pltpu.SMEM(umklapp.shape, jnp.int32),
            pltpu.VMEM((2, nstore, PREP, cols), jnp.bfloat16),
            pltpu.VMEM((2, nstore, rows - PREP, cols), jnp.bfloat16),
            side, side, side, side, side,
            tile, tile, tile, tile, tile,
            pltpu.SemaphoreType.DMA((4,)),
            pltpu.SemaphoreType.DMA((1,)),
            pltpu.SemaphoreType.DMA((2 + pieces // Z_GROUP,)),
            pltpu.SemaphoreType.DMA((1,)),
            pltpu.SemaphoreType.DMA((pieces // X_GROUP,)),
            pltpu.SemaphoreType.DMA((3,)),
            pltpu.SemaphoreType.DMA((3,)),
        ],
        compiler_params=pltpu.CompilerParams(
            collective_id=0, has_side_effects=True, vmem_limit_bytes=56 * 1024 * 1024
        ),
    )(block, bands, umklapp)
    flux, links = pl.pallas_call(
        split,
        out_shape=(
            jax.ShapeDtypeStruct((1, 1, 2), jnp.float32),
            jax.ShapeDtypeStruct((1, 1, 2, 3), jnp.float32),
        ),
        in_specs=[pl.BlockSpec(memory_space=pltpu.VMEM)],
        out_specs=(
            pl.BlockSpec(memory_space=pltpu.VMEM),
            pl.BlockSpec(memory_space=pltpu.VMEM),
        ),
        compiler_params=pltpu.CompilerParams(vmem_limit_bytes=1024 * 1024),
    )(found)
    return (flux, jnp.swapaxes(links, 2, 3))


def solution(mesh):
    in_specs = (P("kx", "ky", None, None, None, None), P(), P())
    out_specs = (P("kx", "ky", None), P("kx", "ky", None, None))
    return jax.shard_map(
        per_device, mesh=mesh, in_specs=in_specs, out_specs=out_specs, check_vma=False
    )
```
